32 devices in a mesh: dp: 8 (over y, x, core), pipe: 4 (over z).
Axes of the slice: x: 2, y: 2, z: 4, core: 2. Of those that a mesh axis runs over, the one named last changes fastest.
Arguments:
- embed_grad: bfloat16 [512, 4608], P('dp', 'pipe'), may hold values from -0.35 to 0.35
- ids: int32 [512], P('dp'), may hold values from 0 to 11263
Outputs:
- table_grad: float32 [11264, 4608], P('dp', 'pipe')
The draws below stay inside these ranges and needn't reach their ends.
All inputs are finite; a program needn't handle non-finite values.
Results may differ from the reference program's by a relative error of at most 0.00035.
Values may be sent and summed in bfloat16 or wider, within the bound.
A program may use at most 64 MiB of HBM per device.

```python
import math
import jax
import jax.numpy as jnp
import numpy as np
from jax import lax

D = 4608
VOC_DEV = 1408
TOKENS = 512
VOCAB = 11264
N_DP = 8


def draw_embed_grad(key, part):
    rows = jnp.arange(TOKENS, dtype=jnp.float32)[:, None] / TOKENS
    columns = jnp.arange(D, dtype=jnp.float32)[None, :] / D
    noise = jnp.clip(jax.random.normal(key, (TOKENS, D), jnp.float32), -5.0, 5.0)
    scale = 0.015 * jnp.exp(jnp.log(3.0) * rows) * jnp.exp(jnp.log(1.5) * columns)
    values = noise * scale
    return jnp.clip(values, -0.35, 0.35).astype(jnp.bfloat16)


def with_ends(drawn, key, low, high):
    longest = drawn.shape.index(max(drawn.shape))
    spots = []
    for shift in (0, 1):
        where = [jax.random.randint(jax.random.fold_in(key, axis), (), 0, length) for axis, length in enumerate(drawn.shape)]
        where[longest] = (where[longest] + shift) % drawn.shape[longest]
        spots.append(tuple(where))
    return drawn.at[spots[0]].set(low).at[spots[1]].set(high)


def rank_bounds(amount, slope):
    weights = [(1 << 20) // math.isqrt(standing ** slope) + 1 for standing in range(1, amount + 1)]
    width = 1 + sum(weights) // (1 << 30)
    return np.cumsum(np.array([max(1, weight // width) for weight in weights]))


def ranked_ids(key, extent, amount, lean):
    table = rank_bounds(amount, lean)
    lot = jax.random.randint(jax.random.fold_in(key, 1), extent, 0, int(table[amount - 1]))
    standing = jnp.searchsorted(jnp.asarray(table, jnp.int32), lot, side="right")
    return jax.random.permutation(jax.random.fold_in(key, 2), amount)[standing].astype(jnp.int32)


def setup_inputs(seed: int = 0) -> dict:
    seeds = jax.random.split(jax.random.key(seed), 3)
    embed_grad = draw_embed_grad(jax.random.fold_in(seeds[2], 71), 0)
    ids = with_ends(ranked_ids(seeds[1], (TOKENS,), VOCAB, 2), jax.random.fold_in(seeds[1], 3), 0, VOCAB - 1).astype(jnp.int32)
    return dict(embed_grad=embed_grad, ids=ids)


def reference(embed_grad, ids):
    cotangent = embed_grad.astype(jnp.float32)

    def block_rows(block_index):
        start = block_index * VOC_DEV
        local = ids - start
        inside = (local >= 0) & (local < VOC_DEV)
        segment = jnp.where(inside, local, VOC_DEV).astype(jnp.int32)
        summed = jax.ops.segment_sum(cotangent, segment, VOC_DEV + 1)
        return summed[:VOC_DEV] * math.sqrt(D)
    grad_rows = lax.map(block_rows, jnp.arange(N_DP, dtype=jnp.int32))
    grad_norm = jnp.sqrt(jnp.sum(grad_rows * grad_rows) + 1e-06)
    factor = jnp.minimum(1.0, 0.2 * math.sqrt(TOKENS * D) / grad_norm)
    return (grad_rows * factor).reshape(VOCAB, D)
```

```python
import functools
import math

import jax
import jax.numpy as jnp
from jax import lax
from jax.experimental import pallas as pl
from jax.experimental.pallas import tpu as pltpu
from jax.sharding import PartitionSpec as P

VOC_DEV = 1408
CHUNKS = 3
STRIPES = 8
MESH = pl.DeviceIdType.MESH


def gather_kernel(n_dp, n_pipe, clip, scale, grad_ref, ids_ref, made_ref, factor_ref,
                  held, id_held, gathered, first, hot, sums, load_sem, late_sem, far_sem, line_sem,
                  send_sem, recv_sem, id_sem, part_sem, sum_sem):
    me = lax.axis_index("dp")
    z = lax.axis_index("pipe")
    chip, core = me // 2, lax.rem(me, 2)
    to_sibling = 1 - 2 * core
    to_x = 2 - 4 * lax.rem(chip, 2)
    to_y = 4 - 8 * (chip // 2)
    sibling, x_peer, y_peer = me + to_sibling, me + to_x, me + to_y
    diagonal = me + to_x + to_y
    relayed = me + (1 - core) * to_x + core * to_y
    relay_to = me + core * to_x + (1 - core) * to_y
    chunks, _, count, tile = held.shape
    tokens = n_dp * count
    last_chip = n_dp // 2 - 1
    late = chip == last_chip
    collects = (core == 1) & (chip < chunks)

    def collector(part):
        return 2 * part + 1

    load_ids = pltpu.make_async_copy(ids_ref, id_held.at[me], load_sem.at[0])
    load_ids.start()
    for part in range(chunks):
        columns = grad_ref.at[:, pl.ds(part * tile, tile)]
        pltpu.make_async_copy(columns, held.at[part, me], load_sem.at[1]).start()
        pl.when(me == collector(part))(
            pltpu.make_async_copy(columns, gathered.at[me], part_sem.at[1]).start
        )

    def taken(ref, semaphore):
        pltpu.make_async_copy(ref, ref, semaphore).wait()

    barrier = pltpu.get_barrier_semaphore()

    def greet(semaphore, device, plane):
        pl.semaphore_signal(semaphore, inc=1, device_id=(device, plane), device_id_type=MESH)

    greet(barrier, sibling, z)

    @pl.when(chip < last_chip)
    def _():
        for ahead in range(2, n_dp, 2):
            for other in range(2):
                greet(barrier, lax.rem(2 * chip + ahead, n_dp) + other, z)

    for other in range(1, n_pipe):
        @pl.when(z < other)
        def _():
            greet(barrier, me, other)
    with jax.named_scope("barrier"):
        pl.semaphore_wait(barrier, jnp.where(late, n_dp - 1, n_dp - 3) + z)
    load_ids.wait()

    @pl.when(late)
    def _():
        for other in range(n_dp - 2):
            greet(late_sem, other, z)

    for other in range(n_pipe - 1):
        @pl.when(z > other)
        def _():
            greet(far_sem, me, other)

    def id_copy(ahead):
        return pltpu.make_async_remote_copy(
            src_ref=id_held.at[me], dst_ref=id_held.at[me],
            send_sem=id_sem.at[0], recv_sem=id_sem.at[1],
            device_id=(lax.rem(me + ahead, n_dp), z), device_id_type=MESH,
        )

    for ahead in range(1, n_dp):
        early = (lax.rem(me + ahead, n_dp) // 2 < last_chip) | late
        pl.when(early)(lambda ahead=ahead: id_copy(ahead).start())

    def part_copy(part):
        return pltpu.make_async_remote_copy(
            src_ref=held.at[part, me], dst_ref=gathered.at[me],
            send_sem=part_sem.at[0], recv_sem=part_sem.at[1],
            device_id=(collector(part), z), device_id_type=MESH,
        )

    taken(held.at[:, me], load_sem.at[1])
    for part in range(chunks):
        pl.when(me != collector(part))(lambda part=part: part_copy(part).start())

    def copy(block, part, target, place):
        return pltpu.make_async_remote_copy(
            src_ref=held.at[part, block], dst_ref=held.at[part, block],
            send_sem=send_sem.at[0], recv_sem=recv_sem.at[place, part],
            device_id=(target, z), device_id_type=MESH,
        )

    def arrived(place, part, count=1):
        taken(held.at[part, pl.ds(0, count)], recv_sem.at[place, part])

    own = [(relay_to, 0), (relayed, 1)]

    def send_own(part):
        for target, place in own:
            pl.when(late | (target // 2 < last_chip))(copy(me, part, target, place).start)

    def send_late(part):
        for target, place in own:
            pl.when(target // 2 == last_chip)(copy(me, part, target, place).start)

    send_own(0)
    with jax.named_scope("late"):
        @pl.when(chip < last_chip)
        def _():
            pl.semaphore_wait(late_sem, 2)
            for ahead in range(1, n_dp):
                pl.when(lax.rem(me + ahead, n_dp) // 2 == last_chip)(
                    lambda ahead=ahead: id_copy(ahead).start()
                )
            send_late(0)
    for part in range(1, chunks):
        send_own(part)
        pl.when(chip < last_chip)(lambda part=part: send_late(part))
    for part in range(chunks):
        copy(me, part, sibling, 3).start()

    with jax.named_scope("far"):
        @pl.when(z < n_pipe - 1)
        def _():
            pl.semaphore_wait(far_sem, n_pipe - 1 - z)
    for part in range(chunks):
        pl.when(me != collector(part))(lambda part=part: greet(line_sem, collector(part), z))

    with jax.named_scope("ids"):
        taken(id_held.at[pl.ds(0, n_dp - 1)], id_sem.at[1])
    ids = jnp.concatenate([id_held[block] for block in range(n_dp)], axis=1)

    def sum_copy(ahead, up, slot):
        return pltpu.make_async_remote_copy(
            src_ref=sums.at[slot], dst_ref=sums.at[slot],
            send_sem=sum_sem.at[0], recv_sem=sum_sem.at[1],
            device_id=(lax.rem(me + ahead, n_dp), lax.rem(z + up, n_pipe)), device_id_type=MESH,
        )

    targets = [
        (ahead, up % n_pipe) for up in range(1, n_pipe + 1) for ahead in range(n_dp)
        if ahead or up < n_pipe
    ]
    my_slot = chip * n_pipe + z

    @pl.when(collects)
    def _():
        columns = []
        for start in range(0, tokens, 128):
            columns.append(
                jnp.broadcast_to(ids[:, start:start + 128].astype(jnp.float32), (128, 128)).T[:, :1]
            )
        column = jnp.concatenate(columns, axis=0)
        same = jnp.where(column == ids.astype(jnp.float32), 1.0, 0.0)
        here = lax.broadcasted_iota(jnp.int32, same.shape, 0)
        other = lax.broadcasted_iota(jnp.int32, same.shape, 1)
        earlier = jnp.sum(jnp.where(other < here, same, 0.0), axis=1, keepdims=True)
        first[...] = jnp.where(earlier == 0.0, same, 0.0).astype(jnp.bfloat16)
        with jax.named_scope("parts"):
            taken(gathered, part_sem.at[1])
        summed = jnp.dot(
            first[...], gathered[...].reshape(tokens, tile), preferred_element_type=jnp.float32
        )
        squares = jnp.sum(summed * summed, axis=0, keepdims=True)
        total = squares[:, :128]
        for lane in range(128, tile, 128):
            total = total + squares[:, lane:lane + 128]
        sums[my_slot] = total
        with jax.named_scope("line"):
            pl.semaphore_wait(line_sem, n_dp - 1)
        with jax.named_scope("share"):
            for ahead, up in targets:
                sum_copy(ahead, up, my_slot).start()

    for part in range(chunks):
        with jax.named_scope("relay"):
            arrived(1, part)
            copy(relayed, part, relay_to, 2).start()
            copy(relayed, part, sibling, 3).start()
            arrived(0, part)
            copy(relay_to, part, sibling, 3).start()

    vocab = made_ref.shape[0]
    wanted = lax.broadcasted_iota(jnp.int32, (vocab, tokens), 0) + me * vocab
    hot[...] = jnp.where(wanted == ids, 1.0, 0.0).astype(jnp.bfloat16)

    def forward(part):
        with jax.named_scope("diagonal"):
            arrived(2, part)
            copy(diagonal, part, sibling, 3).start()

    def make(part):
        with jax.named_scope("rest"):
            arrived(3, part, n_dp // 2)
        made_ref[:, part * tile:(part + 1) * tile] = jnp.dot(
            hot[...], held[part].reshape(tokens, tile), preferred_element_type=jnp.float32
        )

    forward(0)
    for part in range(1, chunks):
        forward(part)
        make(part - 1)
    make(chunks - 1)

    taken(held.at[:, pl.ds(0, n_dp - 1)], send_sem.at[0])
    taken(id_held.at[pl.ds(0, n_dp - 1)], id_sem.at[0])
    partials = chunks * n_pipe

    @pl.when(collects)
    def _():
        taken(gathered.at[pl.ds(0, chunks - 1)], part_sem.at[0])
        taken(sums.at[pl.ds(0, n_dp * n_pipe - 1)], sum_sem.at[0])
        with jax.named_scope("sums"):
            taken(sums.at[pl.ds(0, partials - 1)], sum_sem.at[1])

    @pl.when(jnp.logical_not(collects))
    def _():
        taken(gathered.at[pl.ds(0, chunks)], part_sem.at[0])
        with jax.named_scope("sums"):
            taken(sums.at[pl.ds(0, partials)], sum_sem.at[1])

    whole = sums[0]
    for slot in range(1, partials):
        whole = whole + sums[slot]
    norm = jnp.sqrt(jnp.sum(whole, axis=1, keepdims=True) * (scale * scale) + 1e-06)
    factor = jnp.minimum(1.0, clip / norm) * scale
    factor_ref[...] = jnp.broadcast_to(factor, factor_ref.shape)


def rows_kernel(factor_ref, made_ref, out_ref, scaled, sem):
    height = scaled.shape[0] // STRIPES
    factor = factor_ref[:, :1]
    for stripe in range(STRIPES):
        where = pl.ds(stripe * height, height)
        scaled[where] = made_ref[where] * factor
        pltpu.make_async_copy(scaled.at[where], out_ref.at[where], sem.at[0]).start()
    pltpu.make_async_copy(scaled, out_ref, sem.at[0]).wait()


def rows_of(made, factor):
    vmem = pl.BlockSpec(memory_space=pltpu.VMEM)
    return pl.pallas_call(
        rows_kernel,
        out_shape=jax.ShapeDtypeStruct(made.shape, jnp.float32),
        in_specs=[vmem, vmem],
        out_specs=pl.BlockSpec(memory_space=pltpu.HBM),
        scratch_shapes=[
            pltpu.VMEM(made.shape, jnp.float32),
            pltpu.SemaphoreType.DMA((1,)),
        ],
        compiler_params=pltpu.CompilerParams(vmem_limit_bytes=24 * 2**20),
        name="rows",
    )(factor, made)


def per_device(embed_grad, ids):
    n_dp, n_pipe = lax.axis_size("dp"), lax.axis_size("pipe")
    count, width = embed_grad.shape
    features = width * n_pipe
    tokens = count * n_dp
    tile = width // CHUNKS
    vmem = pl.BlockSpec(memory_space=pltpu.VMEM)
    hbm = pl.BlockSpec(memory_space=pltpu.HBM)
    made, factor = pl.pallas_call(
        functools.partial(
            gather_kernel, n_dp, n_pipe, 0.2 * math.sqrt(tokens * features), math.sqrt(features)
        ),
        out_shape=(
            pltpu.VMEM((VOC_DEV, width), jnp.float32),
            pltpu.VMEM((1, 128), jnp.float32),
        ),
        in_specs=[hbm, hbm],
        out_specs=(vmem, vmem),
        scratch_shapes=[
            pltpu.VMEM((CHUNKS, n_dp, count, tile), embed_grad.dtype),
            pltpu.VMEM((n_dp, 1, count), jnp.int32),
            pltpu.VMEM((n_dp, count, tile), embed_grad.dtype),
            pltpu.VMEM((tokens, tokens), jnp.bfloat16),
            pltpu.VMEM((VOC_DEV, tokens), jnp.bfloat16),
            pltpu.VMEM((n_dp * n_pipe, 1, 128), jnp.float32),
            pltpu.SemaphoreType.DMA((2,)),
            pltpu.SemaphoreType.REGULAR,
            pltpu.SemaphoreType.REGULAR,
            pltpu.SemaphoreType.REGULAR,
            pltpu.SemaphoreType.DMA((1,)),
            pltpu.SemaphoreType.DMA((4, CHUNKS)),
            pltpu.SemaphoreType.DMA((2,)),
            pltpu.SemaphoreType.DMA((2,)),
            pltpu.SemaphoreType.DMA((2,)),
        ],
        compiler_params=pltpu.CompilerParams(
            collective_id=0, has_side_effects=True, vmem_limit_bytes=32 * 2**20
        ),
        name="gather",
    )(
        pltpu.with_memory_space_constraint(embed_grad, pltpu.HBM),
        pltpu.with_memory_space_constraint(ids.reshape(1, count), pltpu.HBM),
    )
    return rows_of(made, factor)


def per_device_any(embed_grad, ids):
    tokens_all = embed_grad.shape[0] * lax.axis_size("dp")
    features = embed_grad.shape[1] * lax.axis_size("pipe")
    offset = lax.axis_index("dp") * VOC_DEV
    cotangent_all = lax.all_gather(embed_grad, "dp", axis=0, tiled=True)
    local = lax.all_gather(ids, "dp", axis=0, tiled=True) - offset
    inside = (local >= 0) & (local < VOC_DEV)
    segment = jnp.where(inside, local, VOC_DEV).astype(jnp.int32)
    summed = jax.ops.segment_sum(cotangent_all.astype(jnp.float32), segment, VOC_DEV + 1)
    grad_rows = summed[:VOC_DEV] * math.sqrt(features)
    total = lax.psum(jnp.sum(grad_rows * grad_rows), ("dp", "pipe"))
    grad_norm = jnp.sqrt(total + 1e-06)
    return grad_rows * jnp.minimum(1.0, 0.2 * math.sqrt(tokens_all * features) / grad_norm)


def solution(mesh):
    placed = (P("dp", "pipe"), P("dp"))
    cube = mesh.shape["dp"] == 2 * 2 * 2
    return jax.shard_map(
        per_device if cube else per_device_any, mesh=mesh, in_specs=placed,
        out_specs=P("dp", "pipe"), check_vma=False,
    )
```

```python
import functools
import math

import jax
import jax.numpy as jnp
from jax import lax
from jax.experimental import pallas as pl
from jax.experimental.pallas import tpu as pltpu
from jax.sharding import PartitionSpec as P

VOC_DEV = 1408
CHUNKS = 3
STRIPES = 44
MESH = pl.DeviceIdType.MESH


def count_sends(device, n_dp, chunks):
    chip, core = device // 2, device % 2
    to_x, to_y = 2 - 4 * (chip % 2), 4 - 8 * (chip // 2)
    relay_to, relayed = (device + to_x, device + to_y)[::1 if core else -1]
    pieces = 0
    for part in range(chunks):
        pieces += device != 2 * part + 1
        pieces += (relay_to // 2 != part) + (relayed // 2 != part)
        pieces += chip != part or core == 1
        if chip != part:
            pieces += (relay_to // 2 != part) + 3
        elif core == 1:
            pieces += n_dp
    return pieces


def gather_kernel(n_dp, n_pipe, clip, scale, grad_ref, ids_ref, made_ref, factor_ref,
                  held, id_held, first, hot, sums, load_sem, late_sem, far_sem, line_sem,
                  send_sem, recv_sem, id_sem, part_sem, sum_sem):
    me = lax.axis_index("dp")
    z = lax.axis_index("pipe")
    chip, core = me // 2, lax.rem(me, 2)
    to_sibling = 1 - 2 * core
    to_x = 2 - 4 * lax.rem(chip, 2)
    to_y = 4 - 8 * (chip // 2)
    sibling, x_peer, y_peer = me + to_sibling, me + to_x, me + to_y
    diagonal = me + to_x + to_y
    relayed = me + (1 - core) * to_x + core * to_y
    relay_to = me + core * to_x + (1 - core) * to_y
    _, count, tile = held.shape
    chunks = grad_ref.shape[1] // tile
    tokens = n_dp * count
    last_chip = n_dp // 2 - 1
    late = chip == last_chip
    collects = (core == 1) & (chip < chunks)

    def collector(part):
        return 2 * part + 1

    def slot(part, block):
        return part * n_dp + block

    load_ids = pltpu.make_async_copy(ids_ref, id_held.at[me], load_sem.at[0])
    load_ids.start()
    for part in range(chunks):
        columns = grad_ref.at[:, pl.ds(part * tile, tile)]
        pltpu.make_async_copy(columns, held.at[slot(part, me)], load_sem.at[1]).start()

    def taken(ref, semaphore):
        pltpu.make_async_copy(ref, ref, semaphore).wait()

    barrier = pltpu.get_barrier_semaphore()

    def greet(semaphore, device, plane):
        pl.semaphore_signal(semaphore, inc=1, device_id=(device, plane), device_id_type=MESH)

    greet(barrier, sibling, z)

    @pl.when(chip < last_chip)
    def _():
        for ahead in range(2, n_dp, 2):
            for other in range(2):
                greet(barrier, lax.rem(2 * chip + ahead, n_dp) + other, z)

    for other in range(1, n_pipe):
        @pl.when(z < other)
        def _():
            greet(barrier, me, other)
    with jax.named_scope("barrier"):
        pl.semaphore_wait(barrier, jnp.where(late, n_dp - 1, n_dp - 3) + z)
    load_ids.wait()

    @pl.when(late)
    def _():
        for other in range(n_dp - 2):
            greet(late_sem, other, z)

    for other in range(n_pipe - 1):
        @pl.when(z > other)
        def _():
            greet(far_sem, me, other)

    def id_copy(ahead):
        return pltpu.make_async_remote_copy(
            src_ref=id_held.at[me], dst_ref=id_held.at[me],
            send_sem=id_sem.at[0], recv_sem=id_sem.at[1],
            device_id=(lax.rem(me + ahead, n_dp), z), device_id_type=MESH,
        )

    for ahead in range(1, n_dp):
        early = (lax.rem(me + ahead, n_dp) // 2 < last_chip) | late
        pl.when(early)(lambda ahead=ahead: id_copy(ahead).start())

    def copy_by(block, part, target, semaphore):
        return pltpu.make_async_remote_copy(
            src_ref=held.at[slot(part, block)], dst_ref=held.at[slot(part, block)],
            send_sem=send_sem.at[0], recv_sem=semaphore,
            device_id=(target, z), device_id_type=MESH,
        )

    def copy(block, part, target, place):
        return copy_by(block, part, target, recv_sem.at[place, part])

    def arrived(place, part, pieces=1):
        taken(held.at[pl.ds(0, pieces)], recv_sem.at[place, part])

    taken(held.at[pl.ds(0, chunks)], load_sem.at[1])
    for part in range(chunks):
        pl.when(me != collector(part))(copy_by(me, part, collector(part), part_sem.at[0]).start)

    own = [(relay_to, 0), (relayed, 1)]

    def send_own(part):
        for target, place in own:
            pl.when((target // 2 != part) & (late | (target // 2 < last_chip)))(
                copy(me, part, target, place).start
            )

    def send_late(part):
        for target, place in own:
            pl.when(target // 2 == last_chip)(copy(me, part, target, place).start)

    send_own(0)
    with jax.named_scope("late"):
        @pl.when(chip < last_chip)
        def _():
            pl.semaphore_wait(late_sem, 2)
            for ahead in range(1, n_dp):
                pl.when(lax.rem(me + ahead, n_dp) // 2 == last_chip)(
                    lambda ahead=ahead: id_copy(ahead).start()
                )
            send_late(0)
    for part in range(1, chunks):
        send_own(part)
        pl.when(chip < last_chip)(lambda part=part: send_late(part))
    for part in range(chunks):
        pl.when((chip != part) | (core == 1))(copy(me, part, sibling, 3).start)

    with jax.named_scope("far"):
        @pl.when(z < n_pipe - 1)
        def _():
            pl.semaphore_wait(far_sem, n_pipe - 1 - z)
    for part in range(chunks):
        pl.when(me != collector(part))(lambda part=part: greet(line_sem, collector(part), z))

    with jax.named_scope("ids"):
        taken(id_held.at[pl.ds(0, n_dp - 1)], id_sem.at[1])
    ids = jnp.concatenate([id_held[block] for block in range(n_dp)], axis=1)

    def sum_copy(ahead, up, share):
        return pltpu.make_async_remote_copy(
            src_ref=sums.at[share], dst_ref=sums.at[share],
            send_sem=sum_sem.at[0], recv_sem=sum_sem.at[1],
            device_id=(lax.rem(me + ahead, n_dp), lax.rem(z + up, n_pipe)), device_id_type=MESH,
        )

    targets = [
        (ahead, up % n_pipe) for up in range(1, n_pipe + 1) for ahead in range(n_dp)
        if ahead or up < n_pipe
    ]
    my_slot = chip * n_pipe + z

    @pl.when(collects)
    def _():
        columns = []
        for start in range(0, tokens, 128):
            columns.append(
                jnp.broadcast_to(ids[:, start:start + 128].astype(jnp.float32), (128, 128)).T[:, :1]
            )
        column = jnp.concatenate(columns, axis=0)
        same = jnp.where(column == ids.astype(jnp.float32), 1.0, 0.0)
        here = lax.broadcasted_iota(jnp.int32, same.shape, 0)
        other = lax.broadcasted_iota(jnp.int32, same.shape, 1)
        earlier = jnp.sum(jnp.where(other < here, same, 0.0), axis=1, keepdims=True)
        first[...] = jnp.where(earlier == 0.0, same, 0.0).astype(jnp.bfloat16)
        with jax.named_scope("parts"):
            taken(held.at[pl.ds(0, n_dp - 1)], part_sem.at[0])
        summed = jnp.dot(
            first[...], held[pl.ds(chip * n_dp, n_dp)].reshape(tokens, tile),
            preferred_element_type=jnp.float32,
        )
        squares = jnp.sum(summed * summed, axis=0, keepdims=True)
        total = squares[:, :128]
        for lane in range(128, tile, 128):
            total = total + squares[:, lane:lane + 128]
        sums[my_slot] = total
        with jax.named_scope("line"):
            pl.semaphore_wait(line_sem, n_dp - 1)
        with jax.named_scope("share"):
            for ahead, up in targets:
                sum_copy(ahead, up, my_slot).start()

        copy(sibling + to_x, chip, sibling + to_y, 2).start()
        copy(relayed, chip, relay_to, 2).start()
        for block in (me + to_x, me + to_y, diagonal):
            copy(block, chip, sibling, 3).start()
        for block, place in ((to_y, 0), (to_x, 1), (to_x + to_y, 2)):
            copy(sibling + block, chip, sibling, place).start()

    for part in range(chunks):
        @pl.when(chip != part)
        def _():
            with jax.named_scope("relay"):
                arrived(1, part)
                pl.when(relay_to // 2 != part)(copy(relayed, part, relay_to, 2).start)
                copy(relayed, part, sibling, 3).start()
                arrived(0, part)
                copy(relay_to, part, sibling, 3).start()

    vocab = made_ref.shape[0]
    wanted = lax.broadcasted_iota(jnp.int32, (vocab, tokens), 0) + me * vocab
    hot[...] = jnp.where(wanted == ids, 1.0, 0.0).astype(jnp.bfloat16)

    def forward(part):
        @pl.when(chip != part)
        def _():
            with jax.named_scope("diagonal"):
                arrived(2, part)
                copy(diagonal, part, sibling, 3).start()

    def make(part, start, stop):
        with jax.named_scope("rest"):
            @pl.when((chip == part) & (core == 0))
            def _():
                for place in range(3):
                    arrived(place, part)

            pl.when((chip != part) | (core == 0))(lambda: arrived(3, part, n_dp // 2))
        pieces = []
        for index in range(start // tile, part + 1):
            block = held[pl.ds(index * n_dp, n_dp)].reshape(tokens, tile)
            low, high = max(start - index * tile, 0), min(stop - index * tile, tile)
            pieces.append(block[:, low:high])
        made_ref[:, start:stop] = jnp.dot(
            hot[...], jnp.concatenate(pieces, axis=1), preferred_element_type=jnp.float32
        )

    forward(0)
    done = 0
    for part in range(chunks):
        if part < chunks - 1:
            forward(part + 1)
        stop = (part + 1) * tile
        if part < chunks - 1:
            stop -= stop % 256
        make(part, done, stop)
        done = stop

    counts = [count_sends(device, n_dp, chunks) for device in range(n_dp)]
    for pieces in sorted(set(counts)):
        mine = functools.reduce(
            jnp.logical_or, [me == device for device in range(n_dp) if counts[device] == pieces]
        )
        pl.when(mine)(lambda pieces=pieces: taken(held.at[pl.ds(0, pieces)], send_sem.at[0]))
    taken(id_held.at[pl.ds(0, n_dp - 1)], id_sem.at[0])
    partials = chunks * n_pipe

    @pl.when(collects)
    def _():
        taken(sums.at[pl.ds(0, n_dp * n_pipe - 1)], sum_sem.at[0])
        with jax.named_scope("sums"):
            taken(sums.at[pl.ds(0, partials - 1)], sum_sem.at[1])

    @pl.when(jnp.logical_not(collects))
    def _():
        with jax.named_scope("sums"):
            taken(sums.at[pl.ds(0, partials)], sum_sem.at[1])

    whole = sums[0]
    for slot in range(1, partials):
        whole = whole + sums[slot]
    norm = jnp.sqrt(jnp.sum(whole, axis=1, keepdims=True) * (scale * scale) + 1e-06)
    factor = jnp.minimum(1.0, clip / norm) * scale
    factor_ref[...] = jnp.broadcast_to(factor, factor_ref.shape)


def rows_kernel(factor_ref, made_ref, out_ref, scaled, sem):
    height = scaled.shape[0] // STRIPES
    factor = factor_ref[:, :1]
    for stripe in range(STRIPES):
        where = pl.ds(stripe * height, height)
        scaled[where] = made_ref[where] * factor
        pltpu.make_async_copy(scaled.at[where], out_ref.at[where], sem.at[0]).start()
    pltpu.make_async_copy(scaled, out_ref, sem.at[0]).wait()


def rows_of(made, factor):
    vmem = pl.BlockSpec(memory_space=pltpu.VMEM)
    return pl.pallas_call(
        rows_kernel,
        out_shape=jax.ShapeDtypeStruct(made.shape, jnp.float32),
        in_specs=[vmem, vmem],
        out_specs=pl.BlockSpec(memory_space=pltpu.HBM),
        scratch_shapes=[
            pltpu.VMEM(made.shape, jnp.float32),
            pltpu.SemaphoreType.DMA((1,)),
        ],
        compiler_params=pltpu.CompilerParams(vmem_limit_bytes=24 * 2**20),
        name="rows",
    )(factor, made)


def per_device(embed_grad, ids):
    n_dp, n_pipe = lax.axis_size("dp"), lax.axis_size("pipe")
    count, width = embed_grad.shape
    features = width * n_pipe
    tokens = count * n_dp
    tile = width // CHUNKS
    vmem = pl.BlockSpec(memory_space=pltpu.VMEM)
    hbm = pl.BlockSpec(memory_space=pltpu.HBM)
    made, factor = pl.pallas_call(
        functools.partial(
            gather_kernel, n_dp, n_pipe, 0.2 * math.sqrt(tokens * features), math.sqrt(features)
        ),
        out_shape=(
            pltpu.VMEM((VOC_DEV, width), jnp.float32),
            pltpu.VMEM((1, 128), jnp.float32),
        ),
        in_specs=[hbm, hbm],
        out_specs=(vmem, vmem),
        scratch_shapes=[
            pltpu.VMEM((CHUNKS * n_dp + 4, count, tile), embed_grad.dtype),
            pltpu.VMEM((n_dp, 1, count), jnp.int32),
            pltpu.VMEM((tokens, tokens), jnp.bfloat16),
            pltpu.VMEM((VOC_DEV, tokens), jnp.bfloat16),
            pltpu.VMEM((n_dp * n_pipe, 1, 128), jnp.float32),
            pltpu.SemaphoreType.DMA((2,)),
            pltpu.SemaphoreType.REGULAR,
            pltpu.SemaphoreType.REGULAR,
            pltpu.SemaphoreType.REGULAR,
            pltpu.SemaphoreType.DMA((1,)),
            pltpu.SemaphoreType.DMA((4, CHUNKS)),
            pltpu.SemaphoreType.DMA((2,)),
            pltpu.SemaphoreType.DMA((1,)),
            pltpu.SemaphoreType.DMA((2,)),
        ],
        compiler_params=pltpu.CompilerParams(
            collective_id=0, has_side_effects=True, vmem_limit_bytes=32 * 2**20
        ),
        name="gather",
    )(
        pltpu.with_memory_space_constraint(embed_grad, pltpu.HBM),
        pltpu.with_memory_space_constraint(ids.reshape(1, count), pltpu.HBM),
    )
    return rows_of(made, factor)


def per_device_any(embed_grad, ids):
    tokens_all = embed_grad.shape[0] * lax.axis_size("dp")
    features = embed_grad.shape[1] * lax.axis_size("pipe")
    offset = lax.axis_index("dp") * VOC_DEV
    cotangent_all = lax.all_gather(embed_grad, "dp", axis=0, tiled=True)
    local = lax.all_gather(ids, "dp", axis=0, tiled=True) - offset
    inside = (local >= 0) & (local < VOC_DEV)
    segment = jnp.where(inside, local, VOC_DEV).astype(jnp.int32)
    summed = jax.ops.segment_sum(cotangent_all.astype(jnp.float32), segment, VOC_DEV + 1)
    grad_rows = summed[:VOC_DEV] * math.sqrt(features)
    total = lax.psum(jnp.sum(grad_rows * grad_rows), ("dp", "pipe"))
    grad_norm = jnp.sqrt(total + 1e-06)
    return grad_rows * jnp.minimum(1.0, 0.2 * math.sqrt(tokens_all * features) / grad_norm)


def solution(mesh):
    placed = (P("dp", "pipe"), P("dp"))
    cube = mesh.shape["dp"] == 2 * 2 * 2
    return jax.shard_map(
        per_device if cube else per_device_any, mesh=mesh, in_specs=placed,
        out_specs=P("dp", "pipe"), check_vma=False,
    )
```

```python
import functools
import math

import jax
import jax.numpy as jnp
from jax import lax
from jax.experimental import pallas as pl
from jax.experimental.pallas import tpu as pltpu
from jax.sharding import PartitionSpec as P

VOC_DEV = 1408
CHUNKS = 3
STRIPES = 44
MESH = pl.DeviceIdType.MESH


def count_sends(device, n_dp, chunks):
    chip, core = device // 2, device % 2
    to_x, to_y = 2 - 4 * (chip % 2), 4 - 8 * (chip // 2)
    relay_to, relayed = (device + to_x, device + to_y)[::1 if core else -1]
    pieces = 0
    for part in range(chunks):
        pieces += device != 2 * part + 1
        pieces += (relay_to // 2 != part) + (relayed // 2 != part)
        pieces += chip != part or core == 1
        if chip != part:
            pieces += (relay_to // 2 != part) + 3
        elif core == 1:
            pieces += n_dp
    return pieces


def gather_kernel(n_dp, n_pipe, clip, scale, grad_ref, ids_ref, made_ref, factor_ref,
                  held, id_held, first, hot, sums, load_sem, cross_sem, late_sem, far_sem, line_sem,
                  send_sem, recv_sem, id_sem, part_sem, sum_sem):
    me = lax.axis_index("dp")
    z = lax.axis_index("pipe")
    chip, core = me // 2, lax.rem(me, 2)
    to_sibling = 1 - 2 * core
    to_x = 2 - 4 * lax.rem(chip, 2)
    to_y = 4 - 8 * (chip // 2)
    sibling, x_peer, y_peer = me + to_sibling, me + to_x, me + to_y
    diagonal = me + to_x + to_y
    relayed = me + (1 - core) * to_x + core * to_y
    relay_to = me + core * to_x + (1 - core) * to_y
    _, count, tile = held.shape
    chunks = grad_ref.shape[1] // tile
    tokens = n_dp * count
    last_chip = n_dp // 2 - 1
    late = chip == last_chip
    collects = (core == 1) & (chip < chunks)

    def collector(part):
        return 2 * part + 1

    def slot(part, block):
        return part * n_dp + block

    load_ids = pltpu.make_async_copy(ids_ref, id_held.at[me], load_sem.at[0])
    load_ids.start()
    for part in range(chunks):
        columns = grad_ref.at[:, pl.ds(part * tile, tile)]
        pltpu.make_async_copy(columns, held.at[slot(part, me)], load_sem.at[1]).start()

    def taken(ref, semaphore):
        pltpu.make_async_copy(ref, ref, semaphore).wait()

    barrier = pltpu.get_barrier_semaphore()

    def greet(semaphore, device, plane):
        pl.semaphore_signal(semaphore, inc=1, device_id=(device, plane), device_id_type=MESH)

    greet(barrier, sibling, z)

    leads = chip == 0
    between = jnp.logical_not(leads | late)

    def apart(target):
        return (chip + target // 2 == last_chip) & between

    @pl.when(jnp.logical_not(late))
    def _():
        for ahead in range(2, n_dp, 2):
            target = lax.rem(2 * chip + ahead, n_dp)

            @pl.when(jnp.logical_not(apart(target)))
            def _():
                for other in range(2):
                    greet(barrier, target + other, z)

    for other in range(1, n_pipe):
        @pl.when(z < other)
        def _():
            greet(barrier, me, other)
    with jax.named_scope("barrier"):
        near = jnp.where(leads, n_dp - 3, jnp.where(late, n_dp - 1, 3))
        pl.semaphore_wait(barrier, near + z)

    @pl.when(me == 1)
    def _():
        for target in range(2, n_dp - 2):
            greet(cross_sem, target, z)

    load_ids.wait()

    @pl.when(late)
    def _():
        for other in range(n_dp - 2):
            greet(late_sem, other, z)

    for other in range(n_pipe - 1):
        @pl.when(z > other)
        def _():
            greet(far_sem, me, other)

    def id_copy(ahead):
        return pltpu.make_async_remote_copy(
            src_ref=id_held.at[me], dst_ref=id_held.at[me],
            send_sem=id_sem.at[0], recv_sem=id_sem.at[1],
            device_id=(lax.rem(me + ahead, n_dp), z), device_id_type=MESH,
        )

    for ahead in range(1, n_dp):
        target = lax.rem(me + ahead, n_dp)
        early = ((target // 2 < last_chip) | late) & jnp.logical_not(apart(target))
        pl.when(early)(lambda ahead=ahead: id_copy(ahead).start())

    def copy_by(block, part, target, semaphore):
        return pltpu.make_async_remote_copy(
            src_ref=held.at[slot(part, block)], dst_ref=held.at[slot(part, block)],
            send_sem=send_sem.at[0], recv_sem=semaphore,
            device_id=(target, z), device_id_type=MESH,
        )

    def copy(block, part, target, place):
        return copy_by(block, part, target, recv_sem.at[place, part])

    def arrived(place, part, pieces=1):
        taken(held.at[pl.ds(0, pieces)], recv_sem.at[place, part])

    order = [*range(1, chunks), 0]
    taken(held.at[pl.ds(0, chunks)], load_sem.at[1])
    hurried = late & (core == 0) & (z == 0)
    pl.when(hurried)(copy(me, 1, relayed, 1).start)
    for part in order:
        pl.when((me != collector(part)) & jnp.logical_not(apart(collector(part))))(
            copy_by(me, part, collector(part), part_sem.at[0]).start
        )

    own = [(relay_to, 0), (relayed, 1)]

    def send_own(part):
        for target, place in own:
            pl.when((target // 2 != part) & (late | (target // 2 < last_chip)))(
                copy(me, part, target, place).start
            )

    def send_late(part):
        for target, place in own:
            pl.when(target // 2 == last_chip)(copy(me, part, target, place).start)

    for target, place in own:
        pl.when((target // 2 != 1) & (late | (target // 2 < last_chip)) & jnp.logical_not(hurried))(
            copy(me, 1, target, place).start
        )
    with jax.named_scope("cross"):
        @pl.when(between)
        def _():
            pl.semaphore_wait(cross_sem, 1)
            for ahead in range(1, n_dp):
                pl.when(apart(lax.rem(me + ahead, n_dp)))(
                    lambda ahead=ahead: id_copy(ahead).start()
                )
            for part in range(1, chunks):
                pl.when(apart(collector(part)))(
                    copy_by(me, part, collector(part), part_sem.at[0]).start
                )
    with jax.named_scope("late"):
        @pl.when(chip < last_chip)
        def _():
            pl.semaphore_wait(late_sem, 2)
            for ahead in range(1, n_dp):
                pl.when(lax.rem(me + ahead, n_dp) // 2 == last_chip)(
                    lambda ahead=ahead: id_copy(ahead).start()
                )
            send_late(1)
    for part in order[1:]:
        send_own(part)
        pl.when(chip < last_chip)(lambda part=part: send_late(part))
    for part in order:
        pl.when((chip != part) | (core == 1))(copy(me, part, sibling, 3).start)

    with jax.named_scope("far"):
        @pl.when(z < n_pipe - 1)
        def _():
            pl.semaphore_wait(far_sem, n_pipe - 1 - z)
    for part in range(chunks):
        pl.when(me != collector(part))(lambda part=part: greet(line_sem, collector(part), z))

    with jax.named_scope("ids"):
        taken(id_held.at[pl.ds(0, n_dp - 1)], id_sem.at[1])
    ids = jnp.concatenate([id_held[block] for block in range(n_dp)], axis=1)

    def sum_copy(ahead, up, share):
        return pltpu.make_async_remote_copy(
            src_ref=sums.at[share], dst_ref=sums.at[share],
            send_sem=sum_sem.at[0], recv_sem=sum_sem.at[1],
            device_id=(lax.rem(me + ahead, n_dp), lax.rem(z + up, n_pipe)), device_id_type=MESH,
        )

    targets = [
        (ahead, up % n_pipe) for up in range(1, n_pipe + 1) for ahead in range(n_dp)
        if ahead or up < n_pipe
    ]
    my_slot = chip * n_pipe + z

    @pl.when(collects)
    def _():
        columns = []
        for start in range(0, tokens, 128):
            columns.append(
                jnp.broadcast_to(ids[:, start:start + 128].astype(jnp.float32), (128, 128)).T[:, :1]
            )
        column = jnp.concatenate(columns, axis=0)
        same = jnp.where(column == ids.astype(jnp.float32), 1.0, 0.0)
        here = lax.broadcasted_iota(jnp.int32, same.shape, 0)
        other = lax.broadcasted_iota(jnp.int32, same.shape, 1)
        earlier = jnp.sum(jnp.where(other < here, same, 0.0), axis=1, keepdims=True)
        first[...] = jnp.where(earlier == 0.0, same, 0.0).astype(jnp.bfloat16)
        with jax.named_scope("parts"):
            taken(held.at[pl.ds(0, n_dp - 1)], part_sem.at[0])
        summed = jnp.dot(
            first[...], held[pl.ds(chip * n_dp, n_dp)].reshape(tokens, tile),
            preferred_element_type=jnp.float32,
        )
        squares = jnp.sum(summed * summed, axis=0, keepdims=True)
        total = squares[:, :128]
        for lane in range(128, tile, 128):
            total = total + squares[:, lane:lane + 128]
        sums[my_slot] = total
        with jax.named_scope("line"):
            pl.semaphore_wait(line_sem, n_dp - 1)
        with jax.named_scope("share"):
            for ahead, up in targets:
                sum_copy(ahead, up, my_slot).start()

        copy(sibling + to_x, chip, sibling + to_y, 2).start()
        copy(relayed, chip, relay_to, 2).start()
        for block in (me + to_x, me + to_y, diagonal):
            copy(block, chip, sibling, 3).start()
        for block, place in ((to_y, 0), (to_x, 1), (to_x + to_y, 2)):
            copy(sibling + block, chip, sibling, place).start()

    for part in order:
        @pl.when(chip != part)
        def _():
            with jax.named_scope("relay"):
                arrived(1, part)
                pl.when(relay_to // 2 != part)(copy(relayed, part, relay_to, 2).start)
                copy(relayed, part, sibling, 3).start()
                arrived(0, part)
                copy(relay_to, part, sibling, 3).start()

    vocab = made_ref.shape[0]
    wanted = lax.broadcasted_iota(jnp.int32, (vocab, tokens), 0) + me * vocab
    hot[...] = jnp.where(wanted == ids, 1.0, 0.0).astype(jnp.bfloat16)

    def forward(part):
        @pl.when(chip != part)
        def _():
            with jax.named_scope("diagonal"):
                arrived(2, part)
                copy(diagonal, part, sibling, 3).start()

    def make(part, start, stop):
        with jax.named_scope("rest"):
            @pl.when((chip == part) & (core == 0))
            def _():
                for place in range(3):
                    arrived(place, part)

            pl.when((chip != part) | (core == 0))(lambda: arrived(3, part, n_dp // 2))
        pieces = []
        for index in range(start // tile, -(-stop // tile)):
            block = held[pl.ds(index * n_dp, n_dp)].reshape(tokens, tile)
            low, high = max(start - index * tile, 0), min(stop - index * tile, tile)
            pieces.append(block[:, low:high])
        made_ref[:, start:stop] = jnp.dot(
            hot[...], jnp.concatenate(pieces, axis=1), preferred_element_type=jnp.float32
        )

    def make_all(order, edges):
        forward(order[0])
        for place, part in enumerate(order):
            if place < chunks - 1:
                forward(order[place + 1])
            make(part, *edges[part])

    down = [part * tile - part * tile % 256 for part in range(chunks)] + [chunks * tile]
    edges = [(down[part], down[part + 1]) for part in range(chunks)]
    up = -(-tile // 256) * 256
    pl.when(leads)(lambda: make_all(range(chunks), edges))
    edges = [(0, up), (up, edges[1][1])] + edges[2:]
    pl.when(jnp.logical_not(leads))(lambda: make_all(order, edges))

    counts = [count_sends(device, n_dp, chunks) for device in range(n_dp)]
    for pieces in sorted(set(counts)):
        mine = functools.reduce(
            jnp.logical_or, [me == device for device in range(n_dp) if counts[device] == pieces]
        )
        pl.when(mine)(lambda pieces=pieces: taken(held.at[pl.ds(0, pieces)], send_sem.at[0]))
    taken(id_held.at[pl.ds(0, n_dp - 1)], id_sem.at[0])
    partials = chunks * n_pipe

    @pl.when(collects)
    def _():
        taken(sums.at[pl.ds(0, n_dp * n_pipe - 1)], sum_sem.at[0])
        with jax.named_scope("sums"):
            taken(sums.at[pl.ds(0, partials - 1)], sum_sem.at[1])

    @pl.when(jnp.logical_not(collects))
    def _():
        with jax.named_scope("sums"):
            taken(sums.at[pl.ds(0, partials)], sum_sem.at[1])

    whole = sums[0]
    for slot in range(1, partials):
        whole = whole + sums[slot]
    norm = jnp.sqrt(jnp.sum(whole, axis=1, keepdims=True) * (scale * scale) + 1e-06)
    factor = jnp.minimum(1.0, clip / norm) * scale
    factor_ref[...] = jnp.broadcast_to(factor, factor_ref.shape)


def rows_kernel(factor_ref, made_ref, out_ref, scaled, sem):
    height = scaled.shape[0] // STRIPES
    factor = factor_ref[:, :1]
    for stripe in range(STRIPES):
        where = pl.ds(stripe * height, height)
        scaled[where] = made_ref[where] * factor
        pltpu.make_async_copy(scaled.at[where], out_ref.at[where], sem.at[0]).start()
    pltpu.make_async_copy(scaled, out_ref, sem.at[0]).wait()


def rows_of(made, factor):
    vmem = pl.BlockSpec(memory_space=pltpu.VMEM)
    return pl.pallas_call(
        rows_kernel,
        out_shape=jax.ShapeDtypeStruct(made.shape, jnp.float32),
        in_specs=[vmem, vmem],
        out_specs=pl.BlockSpec(memory_space=pltpu.HBM),
        scratch_shapes=[
            pltpu.VMEM(made.shape, jnp.float32),
            pltpu.SemaphoreType.DMA((1,)),
        ],
        compiler_params=pltpu.CompilerParams(vmem_limit_bytes=24 * 2**20),
        name="rows",
    )(factor, made)


def per_device(embed_grad, ids):
    n_dp, n_pipe = lax.axis_size("dp"), lax.axis_size("pipe")
    count, width = embed_grad.shape
    features = width * n_pipe
    tokens = count * n_dp
    tile = width // CHUNKS
    vmem = pl.BlockSpec(memory_space=pltpu.VMEM)
    hbm = pl.BlockSpec(memory_space=pltpu.HBM)
    made, factor = pl.pallas_call(
        functools.partial(
            gather_kernel, n_dp, n_pipe, 0.2 * math.sqrt(tokens * features), math.sqrt(features)
        ),
        out_shape=(
            pltpu.VMEM((VOC_DEV, width), jnp.float32),
            pltpu.VMEM((1, 128), jnp.float32),
        ),
        in_specs=[hbm, hbm],
        out_specs=(vmem, vmem),
        scratch_shapes=[
            pltpu.VMEM((CHUNKS * n_dp + 4, count, tile), embed_grad.dtype),
            pltpu.VMEM((n_dp, 1, count), jnp.int32),
            pltpu.VMEM((tokens, tokens), jnp.bfloat16),
            pltpu.VMEM((VOC_DEV, tokens), jnp.bfloat16),
            pltpu.VMEM((n_dp * n_pipe, 1, 128), jnp.float32),
            pltpu.SemaphoreType.DMA((2,)),
            pltpu.SemaphoreType.REGULAR,
            pltpu.SemaphoreType.REGULAR,
            pltpu.SemaphoreType.REGULAR,
            pltpu.SemaphoreType.REGULAR,
            pltpu.SemaphoreType.DMA((1,)),
            pltpu.SemaphoreType.DMA((4, CHUNKS)),
            pltpu.SemaphoreType.DMA((2,)),
            pltpu.SemaphoreType.DMA((1,)),
            pltpu.SemaphoreType.DMA((2,)),
        ],
        compiler_params=pltpu.CompilerParams(
            collective_id=0, has_side_effects=True, vmem_limit_bytes=32 * 2**20
        ),
        name="gather",
    )(
        pltpu.with_memory_space_constraint(embed_grad, pltpu.HBM),
        pltpu.with_memory_space_constraint(ids.reshape(1, count), pltpu.HBM),
    )
    return rows_of(made, factor)


def per_device_any(embed_grad, ids):
    tokens_all = embed_grad.shape[0] * lax.axis_size("dp")
    features = embed_grad.shape[1] * lax.axis_size("pipe")
    offset = lax.axis_index("dp") * VOC_DEV
    cotangent_all = lax.all_gather(embed_grad, "dp", axis=0, tiled=True)
    local = lax.all_gather(ids, "dp", axis=0, tiled=True) - offset
    inside = (local >= 0) & (local < VOC_DEV)
    segment = jnp.where(inside, local, VOC_DEV).astype(jnp.int32)
    summed = jax.ops.segment_sum(cotangent_all.astype(jnp.float32), segment, VOC_DEV + 1)
    grad_rows = summed[:VOC_DEV] * math.sqrt(features)
    total = lax.psum(jnp.sum(grad_rows * grad_rows), ("dp", "pipe"))
    grad_norm = jnp.sqrt(total + 1e-06)
    return grad_rows * jnp.minimum(1.0, 0.2 * math.sqrt(tokens_all * features) / grad_norm)


def solution(mesh):
    placed = (P("dp", "pipe"), P("dp"))
    cube = mesh.shape["dp"] == 2 * 2 * 2
    return jax.shard_map(
        per_device if cube else per_device_any, mesh=mesh, in_specs=placed,
        out_specs=P("dp", "pipe"), check_vma=False,
    )
```

```python
import functools
import math

import jax
import jax.numpy as jnp
from jax import lax
from jax.experimental import pallas as pl
from jax.experimental.pallas import tpu as pltpu
from jax.sharding import PartitionSpec as P

VOC_DEV = 1408
CHUNKS = 3
STRIPES = 44
MESH = pl.DeviceIdType.MESH


def count_sends(device, n_dp, chunks):
    chip, core = device // 2, device % 2
    to_x, to_y = 2 - 4 * (chip % 2), 4 - 8 * (chip // 2)
    relay_to, relayed = (device + to_x, device + to_y)[::1 if core else -1]
    pieces = 0
    for part in range(chunks):
        pieces += device != 2 * part + 1
        pieces += (relay_to // 2 != part) + (relayed // 2 != part)
        pieces += chip != part or core == 1
        if chip != part:
            pieces += (relay_to // 2 != part) + 3
        elif core == 1:
            pieces += n_dp
    return pieces


def gather_kernel(n_dp, n_pipe, clip, scale, grad_ref, ids_ref, made_ref, factor_ref,
                  held, id_held, first, begun, hot, sums, load_sem, cross_sem, late_sem, far_sem, line_sem,
                  send_sem, recv_sem, id_sem, part_sem, sum_sem):
    me = lax.axis_index("dp")
    z = lax.axis_index("pipe")
    chip, core = me // 2, lax.rem(me, 2)
    to_sibling = 1 - 2 * core
    to_x = 2 - 4 * lax.rem(chip, 2)
    to_y = 4 - 8 * (chip // 2)
    sibling, x_peer, y_peer = me + to_sibling, me + to_x, me + to_y
    diagonal = me + to_x + to_y
    relayed = me + (1 - core) * to_x + core * to_y
    relay_to = me + core * to_x + (1 - core) * to_y
    _, count, tile = held.shape
    chunks = grad_ref.shape[1] // tile
    tokens = n_dp * count
    last_chip = n_dp // 2 - 1
    late = chip == last_chip
    collects = (core == 1) & (chip < chunks)

    half = n_dp // 2

    def collector(part):
        return 2 * part + 1

    def slot(part, block):
        return part * n_dp + block

    load_ids = pltpu.make_async_copy(ids_ref, id_held.at[me], load_sem.at[0])
    load_ids.start()
    for part in range(chunks):
        columns = grad_ref.at[:, pl.ds(part * tile, tile)]
        pltpu.make_async_copy(columns, held.at[slot(part, me)], load_sem.at[1]).start()

    def taken(ref, semaphore):
        pltpu.make_async_copy(ref, ref, semaphore).wait()

    barrier = pltpu.get_barrier_semaphore()

    def greet(semaphore, device, plane):
        pl.semaphore_signal(semaphore, inc=1, device_id=(device, plane), device_id_type=MESH)

    greet(barrier, sibling, z)

    leads = chip == 0
    between = jnp.logical_not(leads | late)

    def apart(target):
        return (chip + target // 2 == last_chip) & between

    @pl.when(jnp.logical_not(late))
    def _():
        for ahead in range(2, n_dp, 2):
            target = lax.rem(2 * chip + ahead, n_dp)

            @pl.when(jnp.logical_not(apart(target)))
            def _():
                for other in range(2):
                    greet(barrier, target + other, z)

    for other in range(1, n_pipe):
        @pl.when(z < other)
        def _():
            greet(barrier, me, other)
    with jax.named_scope("barrier"):
        near = jnp.where(leads, n_dp - 3, jnp.where(late, n_dp - 1, 3))
        pl.semaphore_wait(barrier, near + z)

    @pl.when(me == 1)
    def _():
        for target in range(2, n_dp - 2):
            greet(cross_sem, target, z)

    load_ids.wait()

    @pl.when(late)
    def _():
        for other in range(n_dp - 2):
            greet(late_sem, other, z)

    for other in range(n_pipe - 1):
        @pl.when(z > other)
        def _():
            greet(far_sem, me, other)

    def id_copy(ahead):
        return pltpu.make_async_remote_copy(
            src_ref=id_held.at[me], dst_ref=id_held.at[me],
            send_sem=id_sem.at[0], recv_sem=id_sem.at[1],
            device_id=(lax.rem(me + ahead, n_dp), z), device_id_type=MESH,
        )

    for ahead in range(1, n_dp):
        target = lax.rem(me + ahead, n_dp)
        early = ((target // 2 < last_chip) | late) & jnp.logical_not(apart(target))
        pl.when(early)(lambda ahead=ahead: id_copy(ahead).start())

    def copy_by(block, part, target, semaphore):
        return pltpu.make_async_remote_copy(
            src_ref=held.at[slot(part, block)], dst_ref=held.at[slot(part, block)],
            send_sem=send_sem.at[0], recv_sem=semaphore,
            device_id=(target, z), device_id_type=MESH,
        )

    def copy(block, part, target, place):
        return copy_by(block, part, target, recv_sem.at[place, part])

    def arrived(place, part, pieces=1):
        taken(held.at[pl.ds(0, pieces)], recv_sem.at[place, part])

    order = [*range(1, chunks), 0]
    taken(held.at[pl.ds(0, chunks)], load_sem.at[1])
    hurried = late & (core == 0) & (z == 0)
    pl.when(hurried)(copy(me, 1, relayed, 1).start)
    for part in order:
        pl.when((me != collector(part)) & jnp.logical_not(apart(collector(part))))(
            copy_by(me, part, collector(part), part_sem.at[me // half]).start
        )

    own = [(relay_to, 0), (relayed, 1)]

    def send_own(part):
        for target, place in own:
            pl.when((target // 2 != part) & (late | (target // 2 < last_chip)))(
                copy(me, part, target, place).start
            )

    def send_late(part):
        for target, place in own:
            pl.when(target // 2 == last_chip)(copy(me, part, target, place).start)

    behind = between & (z > 0)

    def send_first(when):
        for target, place in own:
            pl.when((target // 2 != 1) & (late | (target // 2 < last_chip)) & when)(
                copy(me, 1, target, place).start
            )

    send_first(jnp.logical_not(hurried | behind))
    with jax.named_scope("cross"):
        @pl.when(between)
        def _():
            pl.semaphore_wait(cross_sem, 1)
            for ahead in range(1, n_dp):
                pl.when(apart(lax.rem(me + ahead, n_dp)))(
                    lambda ahead=ahead: id_copy(ahead).start()
                )
            for part in range(1, chunks):
                pl.when(apart(collector(part)))(
                    copy_by(me, part, collector(part), part_sem.at[me // half]).start
                )
    send_first(behind)
    with jax.named_scope("late"):
        @pl.when(chip < last_chip)
        def _():
            pl.semaphore_wait(late_sem, 2)
            for ahead in range(1, n_dp):
                pl.when(lax.rem(me + ahead, n_dp) // 2 == last_chip)(
                    lambda ahead=ahead: id_copy(ahead).start()
                )
            send_late(1)
    for part in order[1:]:
        send_own(part)
        pl.when(chip < last_chip)(lambda part=part: send_late(part))
    for part in order:
        pl.when((chip != part) | (core == 1))(copy(me, part, sibling, 4).start)

    with jax.named_scope("far"):
        @pl.when(z < n_pipe - 1)
        def _():
            pl.semaphore_wait(far_sem, n_pipe - 1 - z)
    for part in range(chunks):
        pl.when(me != collector(part))(lambda part=part: greet(line_sem, collector(part), z))

    with jax.named_scope("ids"):
        taken(id_held.at[pl.ds(0, n_dp - 1)], id_sem.at[1])
    ids = jnp.concatenate([id_held[block] for block in range(n_dp)], axis=1)

    def sum_copy(ahead, up, share):
        return pltpu.make_async_remote_copy(
            src_ref=sums.at[share], dst_ref=sums.at[share],
            send_sem=sum_sem.at[0], recv_sem=sum_sem.at[1],
            device_id=(lax.rem(me + ahead, n_dp), lax.rem(z + up, n_pipe)), device_id_type=MESH,
        )

    targets = [
        (ahead, up % n_pipe) for up in range(1, n_pipe + 1) for ahead in range(n_dp)
        if ahead or up < n_pipe
    ]
    my_slot = chip * n_pipe + z

    @pl.when(collects)
    def _():
        columns = []
        for start in range(0, tokens, 128):
            columns.append(
                jnp.broadcast_to(ids[:, start:start + 128].astype(jnp.float32), (128, 128)).T[:, :1]
            )
        column = jnp.concatenate(columns, axis=0)
        same = jnp.where(column == ids.astype(jnp.float32), 1.0, 0.0)
        here = lax.broadcasted_iota(jnp.int32, same.shape, 0)
        other = lax.broadcasted_iota(jnp.int32, same.shape, 1)
        earlier = jnp.sum(jnp.where(other < here, same, 0.0), axis=1, keepdims=True)
        first[...] = jnp.where(earlier == 0.0, same, 0.0).astype(jnp.bfloat16)
        def summed_of(index):
            with jax.named_scope("parts"):
                mine = me // half == index
                for own in (0, 1):
                    pl.when(mine == (own == 1))(
                        lambda: taken(held.at[pl.ds(0, half - own)], part_sem.at[index])
                    )
            if index == 1:
                for block in (me + to_x, me + to_y, diagonal):
                    copy(block, chip, sibling, 3).start()
                for block, place in ((to_y, 0), (to_x, 1), (to_x + to_y, 2)):
                    copy(sibling + block, chip, sibling, place).start()
            return jnp.dot(
                first[:, index * half * count:(index + 1) * half * count],
                held[pl.ds(chip * n_dp + index * half, half)].reshape(half * count, tile),
                preferred_element_type=jnp.float32,
            )

        begun[...] = summed_of(0)
        summed = begun[...] + summed_of(1)
        squares = jnp.sum(summed * summed, axis=0, keepdims=True)
        total = squares[:, :128]
        for lane in range(128, tile, 128):
            total = total + squares[:, lane:lane + 128]
        sums[my_slot] = total
        with jax.named_scope("line"):
            pl.semaphore_wait(line_sem, n_dp - 1)
        with jax.named_scope("share"):
            for ahead, up in targets:
                sum_copy(ahead, up, my_slot).start()

        copy(sibling + to_x, chip, sibling + to_y, 2).start()
        copy(relayed, chip, relay_to, 2).start()

    for part in order:
        @pl.when(chip != part)
        def _():
            with jax.named_scope("relay"):
                arrived(1, part)
                pl.when(relay_to // 2 != part)(copy(relayed, part, relay_to, 2).start)
                copy(relayed, part, sibling, 3).start()
                arrived(0, part)
                copy(relay_to, part, sibling, 3).start()

    vocab = made_ref.shape[0]
    near_blocks = (me, sibling, relayed, relay_to)
    far_blocks = (sibling + to_x, sibling + to_y, diagonal, sibling + to_x + to_y)
    mixed = jnp.concatenate([id_held[block] for block in near_blocks + far_blocks], axis=1)
    wanted = lax.broadcasted_iota(jnp.int32, (vocab, tokens), 0) + me * vocab
    hot[...] = jnp.where(wanted == mixed, 1.0, 0.0).astype(jnp.bfloat16)

    def stacked(blocks, start, stop):
        pieces = []
        for part in range(start // tile, -(-stop // tile)):
            low, high = max(start - part * tile, 0), min(stop - part * tile, tile)
            pieces.append(jnp.concatenate(
                [held[slot(part, block)][:, low:high] for block in blocks], axis=0
            ))
        return jnp.concatenate(pieces, axis=1)

    with jax.named_scope("near"):
        for part in range(chunks):
            @pl.when((chip == part) & (core == 0))
            def _():
                arrived(0, part)
                arrived(1, part)

            pl.when((chip != part) | (core == 0))(lambda part=part: arrived(4, part))
    made_ref[...] = jnp.dot(
        hot[:, :tokens // 2], stacked(near_blocks, 0, chunks * tile),
        preferred_element_type=jnp.float32,
    )

    def forward(part):
        @pl.when(chip != part)
        def _():
            with jax.named_scope("diagonal"):
                arrived(2, part)
                copy(diagonal, part, sibling, 3).start()

    def make(part, start, stop):
        with jax.named_scope("rest"):
            pl.when((chip == part) & (core == 0))(lambda: arrived(2, part))
            pl.when((chip != part) | (core == 0))(lambda: arrived(3, part, n_dp // 2 - 1))
        made_ref[:, start:stop] += jnp.dot(
            hot[:, tokens // 2:], stacked(far_blocks, start, stop),
            preferred_element_type=jnp.float32,
        )

    def make_all(order, edges):
        forward(order[0])
        for place, part in enumerate(order):
            if place < chunks - 1:
                forward(order[place + 1])
            make(part, *edges[part])

    down = [part * tile - part * tile % 256 for part in range(chunks)] + [chunks * tile]
    edges = [(down[part], down[part + 1]) for part in range(chunks)]
    up = -(-tile // 256) * 256
    pl.when(leads)(lambda: make_all(range(chunks), edges))
    edges = [(0, up), (up, edges[1][1])] + edges[2:]
    pl.when(jnp.logical_not(leads))(lambda: make_all(order, edges))

    counts = [count_sends(device, n_dp, chunks) for device in range(n_dp)]
    for pieces in sorted(set(counts)):
        mine = functools.reduce(
            jnp.logical_or, [me == device for device in range(n_dp) if counts[device] == pieces]
        )
        pl.when(mine)(lambda pieces=pieces: taken(held.at[pl.ds(0, pieces)], send_sem.at[0]))
    taken(id_held.at[pl.ds(0, n_dp - 1)], id_sem.at[0])
    partials = chunks * n_pipe

    @pl.when(collects)
    def _():
        taken(sums.at[pl.ds(0, n_dp * n_pipe - 1)], sum_sem.at[0])
        with jax.named_scope("sums"):
            taken(sums.at[pl.ds(0, partials - 1)], sum_sem.at[1])

    @pl.when(jnp.logical_not(collects))
    def _():
        with jax.named_scope("sums"):
            taken(sums.at[pl.ds(0, partials)], sum_sem.at[1])

    whole = sums[0]
    for slot in range(1, partials):
        whole = whole + sums[slot]
    norm = jnp.sqrt(jnp.sum(whole, axis=1, keepdims=True) * (scale * scale) + 1e-06)
    factor = jnp.minimum(1.0, clip / norm) * scale
    factor_ref[...] = jnp.broadcast_to(factor, factor_ref.shape)


def rows_kernel(factor_ref, made_ref, out_ref, scaled, sem):
    height = scaled.shape[0] // STRIPES
    factor = factor_ref[:, :1]
    for stripe in range(STRIPES):
        where = pl.ds(stripe * height, height)
        scaled[where] = made_ref[where] * factor
        pltpu.make_async_copy(scaled.at[where], out_ref.at[where], sem.at[0]).start()
    pltpu.make_async_copy(scaled, out_ref, sem.at[0]).wait()


def rows_of(made, factor):
    vmem = pl.BlockSpec(memory_space=pltpu.VMEM)
    return pl.pallas_call(
        rows_kernel,
        out_shape=jax.ShapeDtypeStruct(made.shape, jnp.float32),
        in_specs=[vmem, vmem],
        out_specs=pl.BlockSpec(memory_space=pltpu.HBM),
        scratch_shapes=[
            pltpu.VMEM(made.shape, jnp.float32),
            pltpu.SemaphoreType.DMA((1,)),
        ],
        compiler_params=pltpu.CompilerParams(vmem_limit_bytes=24 * 2**20),
        name="rows",
    )(factor, made)


def per_device(embed_grad, ids):
    n_dp, n_pipe = lax.axis_size("dp"), lax.axis_size("pipe")
    count, width = embed_grad.shape
    features = width * n_pipe
    tokens = count * n_dp
    tile = width // CHUNKS
    vmem = pl.BlockSpec(memory_space=pltpu.VMEM)
    hbm = pl.BlockSpec(memory_space=pltpu.HBM)
    made, factor = pl.pallas_call(
        functools.partial(
            gather_kernel, n_dp, n_pipe, 0.2 * math.sqrt(tokens * features), math.sqrt(features)
        ),
        out_shape=(
            pltpu.VMEM((VOC_DEV, width), jnp.float32),
            pltpu.VMEM((1, 128), jnp.float32),
        ),
        in_specs=[hbm, hbm],
        out_specs=(vmem, vmem),
        scratch_shapes=[
            pltpu.VMEM((CHUNKS * n_dp + 4, count, tile), embed_grad.dtype),
            pltpu.VMEM((n_dp, 1, count), jnp.int32),
            pltpu.VMEM((tokens, tokens), jnp.bfloat16),
            pltpu.VMEM((tokens, tile), jnp.float32),
            pltpu.VMEM((VOC_DEV, tokens), jnp.bfloat16),
            pltpu.VMEM((n_dp * n_pipe, 1, 128), jnp.float32),
            pltpu.SemaphoreType.DMA((2,)),
            pltpu.SemaphoreType.REGULAR,
            pltpu.SemaphoreType.REGULAR,
            pltpu.SemaphoreType.REGULAR,
            pltpu.SemaphoreType.REGULAR,
            pltpu.SemaphoreType.DMA((1,)),
            pltpu.SemaphoreType.DMA((5, CHUNKS)),
            pltpu.SemaphoreType.DMA((2,)),
            pltpu.SemaphoreType.DMA((2,)),
            pltpu.SemaphoreType.DMA((2,)),
        ],
        compiler_params=pltpu.CompilerParams(
            collective_id=0, has_side_effects=True, vmem_limit_bytes=32 * 2**20
        ),
        name="gather",
    )(
        pltpu.with_memory_space_constraint(embed_grad, pltpu.HBM),
        pltpu.with_memory_space_constraint(ids.reshape(1, count), pltpu.HBM),
    )
    return rows_of(made, factor)


def per_device_any(embed_grad, ids):
    tokens_all = embed_grad.shape[0] * lax.axis_size("dp")
    features = embed_grad.shape[1] * lax.axis_size("pipe")
    offset = lax.axis_index("dp") * VOC_DEV
    cotangent_all = lax.all_gather(embed_grad, "dp", axis=0, tiled=True)
    local = lax.all_gather(ids, "dp", axis=0, tiled=True) - offset
    inside = (local >= 0) & (local < VOC_DEV)
    segment = jnp.where(inside, local, VOC_DEV).astype(jnp.int32)
    summed = jax.ops.segment_sum(cotangent_all.astype(jnp.float32), segment, VOC_DEV + 1)
    grad_rows = summed[:VOC_DEV] * math.sqrt(features)
    total = lax.psum(jnp.sum(grad_rows * grad_rows), ("dp", "pipe"))
    grad_norm = jnp.sqrt(total + 1e-06)
    return grad_rows * jnp.minimum(1.0, 0.2 * math.sqrt(tokens_all * features) / grad_norm)


def solution(mesh):
    placed = (P("dp", "pipe"), P("dp"))
    cube = mesh.shape["dp"] == 2 * 2 * 2
    return jax.shard_map(
        per_device if cube else per_device_any, mesh=mesh, in_specs=placed,
        out_specs=P("dp", "pipe"), check_vma=False,
    )
```

```python
import functools
import math

import jax
import jax.numpy as jnp
from jax import lax
from jax.experimental import pallas as pl
from jax.experimental.pallas import tpu as pltpu
from jax.sharding import PartitionSpec as P

VOC_DEV = 1408
CHUNKS = 3
STRIPES = 44
MESH = pl.DeviceIdType.MESH


def count_sends(device, n_dp, chunks):
    chip, core = device // 2, device % 2
    to_x, to_y = 2 - 4 * (chip % 2), 4 - 8 * (chip // 2)
    relay_to, relayed = (device + to_x, device + to_y)[::1 if core else -1]
    pieces = 0
    for part in range(chunks):
        pieces += device != 2 * part + 1
        pieces += (relay_to // 2 != part) + (relayed // 2 != part)
        pieces += chip != part or core == 1
        if chip != part:
            pieces += (relay_to // 2 != part) + 3
        elif core == 1:
            pieces += n_dp
    return pieces


def gather_kernel(n_dp, n_pipe, clip, scale, grad_ref, ids_ref, made_ref, factor_ref,
                  held, id_held, first, begun, hot, sums, load_sem, cross_sem, late_sem, far_sem, line_sem,
                  send_sem, recv_sem, twin_sem, id_sem, part_sem, sum_sem):
    me = lax.axis_index("dp")
    z = lax.axis_index("pipe")
    chip, core = me // 2, lax.rem(me, 2)
    to_sibling = 1 - 2 * core
    to_x = 2 - 4 * lax.rem(chip, 2)
    to_y = 4 - 8 * (chip // 2)
    sibling, x_peer, y_peer = me + to_sibling, me + to_x, me + to_y
    diagonal = me + to_x + to_y
    relayed = me + (1 - core) * to_x + core * to_y
    relay_to = me + core * to_x + (1 - core) * to_y
    _, count, tile = held.shape
    chunks = grad_ref.shape[1] // tile
    tokens = n_dp * count
    last_chip = n_dp // 2 - 1
    late = chip == last_chip
    collects = (core == 1) & (chip < chunks)

    half = n_dp // 2

    def collector(part):
        return 2 * part + 1

    def slot(part, block):
        return part * n_dp + block

    load_ids = pltpu.make_async_copy(ids_ref, id_held.at[me], load_sem.at[0])
    load_ids.start()
    for part in range(chunks):
        columns = grad_ref.at[:, pl.ds(part * tile, tile)]
        pltpu.make_async_copy(columns, held.at[slot(part, me)], load_sem.at[1]).start()

    def taken(ref, semaphore):
        pltpu.make_async_copy(ref, ref, semaphore).wait()

    barrier = pltpu.get_barrier_semaphore()

    def greet(semaphore, device, plane):
        pl.semaphore_signal(semaphore, inc=1, device_id=(device, plane), device_id_type=MESH)

    greet(barrier, sibling, z)

    leads = chip == 0
    between = jnp.logical_not(leads | late) & ((z == 0) | (chip == 1))

    def apart(target):
        return (chip + target // 2 == last_chip) & between

    @pl.when(jnp.logical_not(late))
    def _():
        for ahead in range(2, n_dp, 2):
            target = lax.rem(2 * chip + ahead, n_dp)

            opposite = (chip + target // 2 == last_chip) & jnp.logical_not(leads)

            @pl.when(jnp.logical_not(opposite) | ((chip == 1) & (z > 0)))
            def _():
                for other in range(2):
                    greet(barrier, target + other, z)

    for other in range(1, n_pipe):
        @pl.when(z < other)
        def _():
            greet(barrier, me, other)
    with jax.named_scope("barrier"):
        near = jnp.where(between, 3, jnp.where(late, n_dp - 1, n_dp - 3))
        pl.semaphore_wait(barrier, near + z)

    @pl.when(me == 1)
    def _():
        for target in range(2, n_dp - 2):
            pl.when((z == 0) | (target // 2 == 1))(lambda target=target: greet(cross_sem, target, z))

    load_ids.wait()

    @pl.when(late)
    def _():
        for other in range(n_dp - 2):
            greet(late_sem, other, z)

    for other in range(n_pipe - 1):
        @pl.when(z > other)
        def _():
            greet(far_sem, me, other)

    def id_copy(ahead):
        return pltpu.make_async_remote_copy(
            src_ref=id_held.at[me], dst_ref=id_held.at[me],
            send_sem=id_sem.at[0], recv_sem=id_sem.at[1],
            device_id=(lax.rem(me + ahead, n_dp), z), device_id_type=MESH,
        )

    for ahead in range(1, n_dp):
        target = lax.rem(me + ahead, n_dp)
        early = ((target // 2 < last_chip) | late) & jnp.logical_not(apart(target))
        pl.when(early)(lambda ahead=ahead: id_copy(ahead).start())

    def copy_by(block, part, target, semaphore):
        return pltpu.make_async_remote_copy(
            src_ref=held.at[slot(part, block)], dst_ref=held.at[slot(part, block)],
            send_sem=send_sem.at[0], recv_sem=semaphore,
            device_id=(target, z), device_id_type=MESH,
        )

    def copy(block, part, target, place):
        return copy_by(block, part, target, recv_sem.at[place, part])

    def arrived(place, part, pieces=1):
        taken(held.at[pl.ds(0, pieces)], recv_sem.at[place, part])

    order = [*range(1, chunks), 0]
    taken(held.at[pl.ds(0, chunks)], load_sem.at[1])
    hurried = late & (core == 0) & (z == 0)
    pl.when(hurried)(copy(me, 1, relayed, 1).start)
    upper = late & (z > 0)

    def send_part(part, when):
        pl.when((me != collector(part)) & jnp.logical_not(apart(collector(part))) & when)(
            copy_by(me, part, collector(part), part_sem.at[me // half]).start
        )

    send_part(0, upper)
    for part in order:
        send_part(part, jnp.logical_not(upper) if part == 0 else True)

    own = [(relay_to, 0), (relayed, 1)]

    def send_own(part):
        for target, place in own:
            pl.when((target // 2 != part) & (late | (target // 2 < last_chip)))(
                copy(me, part, target, place).start
            )

    def send_late(part):
        for target, place in own:
            pl.when(target // 2 == last_chip)(copy(me, part, target, place).start)

    behind = between & (z > 0)

    def send_first(when):
        for target, place in own:
            pl.when((target // 2 != 1) & (late | (target // 2 < last_chip)) & when)(
                copy(me, 1, target, place).start
            )

    send_first(jnp.logical_not(hurried | behind))
    with jax.named_scope("cross"):
        @pl.when(between)
        def _():
            pl.semaphore_wait(cross_sem, 1)
            for ahead in range(1, n_dp):
                pl.when(apart(lax.rem(me + ahead, n_dp)))(
                    lambda ahead=ahead: id_copy(ahead).start()
                )
            for part in range(1, chunks):
                pl.when(apart(collector(part)))(
                    copy_by(me, part, collector(part), part_sem.at[me // half]).start
                )
    send_first(behind)
    with jax.named_scope("late"):
        @pl.when(chip < last_chip)
        def _():
            pl.semaphore_wait(late_sem, 2)
            for ahead in range(1, n_dp):
                pl.when(lax.rem(me + ahead, n_dp) // 2 == last_chip)(
                    lambda ahead=ahead: id_copy(ahead).start()
                )
            send_late(1)
    for part in order[1:]:
        send_own(part)
        pl.when(chip < last_chip)(lambda part=part: send_late(part))
    for part in order:
        pl.when((chip != part) | (core == 1))(copy_by(me, part, sibling, twin_sem.at[0]).start)

    with jax.named_scope("far"):
        @pl.when(z < n_pipe - 1)
        def _():
            pl.semaphore_wait(far_sem, n_pipe - 1 - z)
    for part in range(chunks):
        pl.when(me != collector(part))(lambda part=part: greet(line_sem, collector(part), z))

    with jax.named_scope("ids"):
        taken(id_held.at[pl.ds(0, n_dp - 1)], id_sem.at[1])
    ids = jnp.concatenate([id_held[block] for block in range(n_dp)], axis=1)

    def sum_copy(ahead, up, share):
        return pltpu.make_async_remote_copy(
            src_ref=sums.at[share], dst_ref=sums.at[share],
            send_sem=sum_sem.at[0], recv_sem=sum_sem.at[1],
            device_id=(lax.rem(me + ahead, n_dp), lax.rem(z + up, n_pipe)), device_id_type=MESH,
        )

    targets = [
        (ahead, up % n_pipe) for up in range(1, n_pipe + 1) for ahead in range(n_dp)
        if ahead or up < n_pipe
    ]
    my_slot = chip * n_pipe + z

    @pl.when(collects)
    def _():
        columns = []
        for start in range(0, tokens, 128):
            columns.append(
                jnp.broadcast_to(ids[:, start:start + 128].astype(jnp.float32), (128, 128)).T[:, :1]
            )
        column = jnp.concatenate(columns, axis=0)
        same = jnp.where(column == ids.astype(jnp.float32), 1.0, 0.0)
        here = lax.broadcasted_iota(jnp.int32, same.shape, 0)
        other = lax.broadcasted_iota(jnp.int32, same.shape, 1)
        earlier = jnp.sum(jnp.where(other < here, same, 0.0), axis=1, keepdims=True)
        first[...] = jnp.where(earlier == 0.0, same, 0.0).astype(jnp.bfloat16)
        def summed_of(index):
            with jax.named_scope("parts"):
                mine = me // half == index
                for own in (0, 1):
                    pl.when(mine == (own == 1))(
                        lambda: taken(held.at[pl.ds(0, half - own)], part_sem.at[index])
                    )
            if index == 1:
                for block in (me + to_x, me + to_y, diagonal):
                    copy(block, chip, sibling, 3).start()
                for block, place in ((to_y, 0), (to_x, 1), (to_x + to_y, 2)):
                    copy(sibling + block, chip, sibling, place).start()
            return jnp.dot(
                first[:, index * half * count:(index + 1) * half * count],
                held[pl.ds(chip * n_dp + index * half, half)].reshape(half * count, tile),
                preferred_element_type=jnp.float32,
            )

        begun[...] = summed_of(0)
        summed = begun[...] + summed_of(1)
        squares = jnp.sum(summed * summed, axis=0, keepdims=True)
        total = squares[:, :128]
        for lane in range(128, tile, 128):
            total = total + squares[:, lane:lane + 128]
        sums[my_slot] = total
        with jax.named_scope("line"):
            pl.semaphore_wait(line_sem, n_dp - 1)
        with jax.named_scope("share"):
            for ahead, up in targets:
                sum_copy(ahead, up, my_slot).start()

        copy(sibling + to_x, chip, sibling + to_y, 2).start()
        copy(relayed, chip, relay_to, 2).start()

    for part in order:
        @pl.when(chip != part)
        def _():
            with jax.named_scope("relay"):
                arrived(1, part)
                pl.when(relay_to // 2 != part)(copy(relayed, part, relay_to, 2).start)
                copy(relayed, part, sibling, 3).start()
                arrived(0, part)
                copy(relay_to, part, sibling, 3).start()

    vocab = made_ref.shape[0]
    near_blocks = (me, sibling, relayed, relay_to)
    far_blocks = (sibling + to_x, sibling + to_y, diagonal, sibling + to_x + to_y)
    mixed = jnp.concatenate([id_held[block] for block in near_blocks + far_blocks], axis=1)
    wanted = lax.broadcasted_iota(jnp.int32, (vocab, tokens), 0) + me * vocab
    hot[...] = jnp.where(wanted == mixed, 1.0, 0.0).astype(jnp.bfloat16)

    def stacked(blocks, start, stop):
        pieces = []
        for part in range(start // tile, -(-stop // tile)):
            low, high = max(start - part * tile, 0), min(stop - part * tile, tile)
            pieces.append(jnp.concatenate(
                [held[slot(part, block)][:, low:high] for block in blocks], axis=0
            ))
        return jnp.concatenate(pieces, axis=1)

    def make_near(parts, start, stop):
        with jax.named_scope("near"):
            for part in parts:
                @pl.when((chip == part) & (core == 0))
                def _():
                    arrived(0, part)
                    arrived(1, part)
        made_ref[:, start:stop] = jnp.dot(
            hot[:, :tokens // 2], stacked(near_blocks, start, stop),
            preferred_element_type=jnp.float32,
        )

    up = -(-tile // 256) * 256
    pl.when(collects)(lambda: taken(held.at[pl.ds(0, chunks - 1)], twin_sem.at[0]))
    pl.when(jnp.logical_not(collects))(lambda: taken(held.at[pl.ds(0, chunks)], twin_sem.at[0]))
    make_near(order[:-1], up, chunks * tile)
    make_near(order[-1:], 0, up)

    def forward(part):
        @pl.when(chip != part)
        def _():
            with jax.named_scope("diagonal"):
                arrived(2, part)
                copy(diagonal, part, sibling, 3).start()

    def make(part, start, stop):
        with jax.named_scope("rest"):
            pl.when((chip == part) & (core == 0))(lambda: arrived(2, part))
            pl.when((chip != part) | (core == 0))(lambda: arrived(3, part, n_dp // 2 - 1))
        made_ref[:, start:stop] += jnp.dot(
            hot[:, tokens // 2:], stacked(far_blocks, start, stop),
            preferred_element_type=jnp.float32,
        )

    def make_all(order, edges, ahead):
        for part in order[:1] if ahead else ():
            make(part, *edges[part])
        for part in order:
            forward(part)
        for part in order[1:] if ahead else order:
            make(part, *edges[part])

    down = [part * tile - part * tile % 256 for part in range(chunks)] + [chunks * tile]
    edges = [(down[part], down[part + 1]) for part in range(chunks)]

    @pl.when(leads)
    def _():
        forward(1)
        make(0, *edges[0])
        for part in range(2, chunks):
            forward(part)
        for part in range(1, chunks):
            make(part, *edges[part])

    last_edges = [(0, up), (up, edges[1][1])] + edges[2:]
    pl.when(late)(lambda: make_all(order, last_edges, False))
    for first_part in range(1, chunks):
        rest_parts = [part for part in order if part != first_part]
        pl.when(chip == first_part)(
            lambda parts=[first_part, *rest_parts]: make_all(parts, last_edges, True)
        )

    counts = [count_sends(device, n_dp, chunks) for device in range(n_dp)]
    for pieces in sorted(set(counts)):
        mine = functools.reduce(
            jnp.logical_or, [me == device for device in range(n_dp) if counts[device] == pieces]
        )
        pl.when(mine)(lambda pieces=pieces: taken(held.at[pl.ds(0, pieces)], send_sem.at[0]))
    taken(id_held.at[pl.ds(0, n_dp - 1)], id_sem.at[0])
    partials = chunks * n_pipe

    @pl.when(collects)
    def _():
        taken(sums.at[pl.ds(0, n_dp * n_pipe - 1)], sum_sem.at[0])
        with jax.named_scope("sums"):
            taken(sums.at[pl.ds(0, partials - 1)], sum_sem.at[1])

    @pl.when(jnp.logical_not(collects))
    def _():
        with jax.named_scope("sums"):
            taken(sums.at[pl.ds(0, partials)], sum_sem.at[1])

    whole = sums[0]
    for slot in range(1, partials):
        whole = whole + sums[slot]
    norm = jnp.sqrt(jnp.sum(whole, axis=1, keepdims=True) * (scale * scale) + 1e-06)
    factor = jnp.minimum(1.0, clip / norm) * scale
    factor_ref[...] = jnp.broadcast_to(factor, factor_ref.shape)


def rows_kernel(factor_ref, made_ref, out_ref, scaled, sem):
    height = scaled.shape[0] // STRIPES
    factor = factor_ref[:, :1]
    for stripe in range(STRIPES):
        where = pl.ds(stripe * height, height)
        scaled[where] = made_ref[where] * factor
        pltpu.make_async_copy(scaled.at[where], out_ref.at[where], sem.at[0]).start()
    pltpu.make_async_copy(scaled, out_ref, sem.at[0]).wait()


def rows_of(made, factor):
    vmem = pl.BlockSpec(memory_space=pltpu.VMEM)
    return pl.pallas_call(
        rows_kernel,
        out_shape=jax.ShapeDtypeStruct(made.shape, jnp.float32),
        in_specs=[vmem, vmem],
        out_specs=pl.BlockSpec(memory_space=pltpu.HBM),
        scratch_shapes=[
            pltpu.VMEM(made.shape, jnp.float32),
            pltpu.SemaphoreType.DMA((1,)),
        ],
        compiler_params=pltpu.CompilerParams(vmem_limit_bytes=24 * 2**20),
        name="rows",
    )(factor, made)


def per_device(embed_grad, ids):
    n_dp, n_pipe = lax.axis_size("dp"), lax.axis_size("pipe")
    count, width = embed_grad.shape
    features = width * n_pipe
    tokens = count * n_dp
    tile = width // CHUNKS
    vmem = pl.BlockSpec(memory_space=pltpu.VMEM)
    hbm = pl.BlockSpec(memory_space=pltpu.HBM)
    made, factor = pl.pallas_call(
        functools.partial(
            gather_kernel, n_dp, n_pipe, 0.2 * math.sqrt(tokens * features), math.sqrt(features)
        ),
        out_shape=(
            pltpu.VMEM((VOC_DEV, width), jnp.float32),
            pltpu.VMEM((1, 128), jnp.float32),
        ),
        in_specs=[hbm, hbm],
        out_specs=(vmem, vmem),
        scratch_shapes=[
            pltpu.VMEM((CHUNKS * n_dp + 4, count, tile), embed_grad.dtype),
            pltpu.VMEM((n_dp, 1, count), jnp.int32),
            pltpu.VMEM((tokens, tokens), jnp.bfloat16),
            pltpu.VMEM((tokens, tile), jnp.float32),
            pltpu.VMEM((VOC_DEV, tokens), jnp.bfloat16),
            pltpu.VMEM((n_dp * n_pipe, 1, 128), jnp.float32),
            pltpu.SemaphoreType.DMA((2,)),
            pltpu.SemaphoreType.REGULAR,
            pltpu.SemaphoreType.REGULAR,
            pltpu.SemaphoreType.REGULAR,
            pltpu.SemaphoreType.REGULAR,
            pltpu.SemaphoreType.DMA((1,)),
            pltpu.SemaphoreType.DMA((4, CHUNKS)),
            pltpu.SemaphoreType.DMA((1,)),
            pltpu.SemaphoreType.DMA((2,)),
            pltpu.SemaphoreType.DMA((2,)),
            pltpu.SemaphoreType.DMA((2,)),
        ],
        compiler_params=pltpu.CompilerParams(
            collective_id=0, has_side_effects=True, vmem_limit_bytes=32 * 2**20
        ),
        name="gather",
    )(
        pltpu.with_memory_space_constraint(embed_grad, pltpu.HBM),
        pltpu.with_memory_space_constraint(ids.reshape(1, count), pltpu.HBM),
    )
    return rows_of(made, factor)


def per_device_any(embed_grad, ids):
    tokens_all = embed_grad.shape[0] * lax.axis_size("dp")
    features = embed_grad.shape[1] * lax.axis_size("pipe")
    offset = lax.axis_index("dp") * VOC_DEV
    cotangent_all = lax.all_gather(embed_grad, "dp", axis=0, tiled=True)
    local = lax.all_gather(ids, "dp", axis=0, tiled=True) - offset
    inside = (local >= 0) & (local < VOC_DEV)
    segment = jnp.where(inside, local, VOC_DEV).astype(jnp.int32)
    summed = jax.ops.segment_sum(cotangent_all.astype(jnp.float32), segment, VOC_DEV + 1)
    grad_rows = summed[:VOC_DEV] * math.sqrt(features)
    total = lax.psum(jnp.sum(grad_rows * grad_rows), ("dp", "pipe"))
    grad_norm = jnp.sqrt(total + 1e-06)
    return grad_rows * jnp.minimum(1.0, 0.2 * math.sqrt(tokens_all * features) / grad_norm)


def solution(mesh):
    placed = (P("dp", "pipe"), P("dp"))
    cube = mesh.shape["dp"] == 2 * 2 * 2
    return jax.shard_map(
        per_device if cube else per_device_any, mesh=mesh, in_specs=placed,
        out_specs=P("dp", "pipe"), check_vma=False,
    )
```
